64 devices in a mesh: dp: 4 (over x, y), ep: 16 (over z, core).
Axes of the slice: x: 2, y: 2, z: 8, core: 2. Of those that a mesh axis runs over, the one named last changes fastest.
The devices are a block of a 4x4x8 slice.
Arguments:
- dispatched: bfloat16 [64, 64, 32, 2048], P('dp', 'ep'), parts along dimension 0
- w_gate: bfloat16 [64, 2048, 1024], P('ep')
- w_up: bfloat16 [64, 2048, 1024], P('ep')
- w_down: bfloat16 [64, 1024, 2048], P('ep')
- fill_count: int32 [64, 64], P('dp', 'ep'), parts along dimension 0
- slot_index: int32 [8192, 8], P(('dp', 'ep')), parts along dimension 0
- expert_id: int32 [8192, 8], P(('dp', 'ep')), parts along dimension 0
- gate_weight: float32 [8192, 8], P(('dp', 'ep')), parts along dimension 0
Outputs:
- output: bfloat16 [8192, 2048], P(('dp', 'ep')), parts along dimension 0
There are 4 independent parts. The reference program is written for one: setup_inputs(seed, part) draws one part's arguments, and reference() takes and returns one part's arrays. A program takes and returns all parts, laid end to end along the dimension named above; an argument that names none is the same for every part.
All inputs are finite; a program needn't handle non-finite values.
Results may differ from the reference program's by a relative error of at most 0.00122.
Values are sent between devices in bfloat16 or wider.
A program may use at most 768 MiB of HBM per device.

```python
import jax
import jax.numpy as jnp
from jax import lax

HIDDEN = 2048
FFN_DIM = 1024
EXPERTS = 64
TOP_K = 8
TOKENS_DEV = 128
GROUP_SIZE = 16
CAPACITY = (2 * TOKENS_DEV * TOP_K) // EXPERTS


def draw_routing(route_key):
    key_perm, key_noise, key_shift = jax.random.split(route_key, 3)
    popularity = jax.random.permutation(key_perm, EXPERTS)
    base_score = 4000 // (popularity + 1)
    noise_term = jax.random.randint(key_noise, (GROUP_SIZE, TOKENS_DEV, EXPERTS), 0, 1000)
    cover_shift = jax.random.randint(key_shift, (GROUP_SIZE, 1), 0, EXPERTS)
    expert_ids = jnp.arange(EXPERTS, dtype=jnp.int32)
    cover_id = (jnp.arange(TOKENS_DEV, dtype=jnp.int32)[None, :] + cover_shift) % EXPERTS
    cover_bonus = jnp.where(expert_ids[None, None, :] == cover_id[:, :, None], 100000, 0)
    route_score = (base_score[None, None, :] + noise_term + cover_bonus) * EXPERTS + expert_ids
    chosen = lax.top_k(route_score, TOP_K)[1]
    onehot = (chosen.reshape(GROUP_SIZE, TOKENS_DEV * TOP_K, 1) == expert_ids).astype(jnp.int32)
    earlier = jnp.cumsum(onehot, axis=1) - onehot
    arrival = jnp.sum(earlier * onehot, axis=2)
    slot_index = jnp.where(arrival < CAPACITY, arrival, -1)
    filled_count = jnp.minimum(jnp.sum(onehot, axis=1), CAPACITY)
    expert_id = chosen.reshape(GROUP_SIZE * TOKENS_DEV, TOP_K).astype(jnp.int32)
    slot_index = slot_index.reshape(GROUP_SIZE * TOKENS_DEV, TOP_K).astype(jnp.int32)
    return expert_id, slot_index, filled_count.astype(jnp.int32)


def setup_inputs(seed: int = 0, part: int = 0) -> dict:
    shared_key, part_root = jax.random.split(jax.random.key(seed))
    key_gate_w, key_up_w, key_down_w = jax.random.split(shared_key, 3)
    part_key = jax.random.fold_in(part_root, part)
    key_route, key_rows, key_mix = jax.random.split(part_key, 3)
    expert_id, slot_index, filled_count = draw_routing(key_route)
    dispatched = jax.random.normal(key_rows, (GROUP_SIZE, EXPERTS, CAPACITY, HIDDEN), jnp.float32)
    w_gate = jax.random.normal(key_gate_w, (EXPERTS, HIDDEN, FFN_DIM), jnp.float32) * HIDDEN ** -0.5
    w_up = jax.random.normal(key_up_w, (EXPERTS, HIDDEN, FFN_DIM), jnp.float32) * HIDDEN ** -0.5
    w_down = jax.random.normal(key_down_w, (EXPERTS, FFN_DIM, HIDDEN), jnp.float32) * FFN_DIM ** -0.5
    logits = jax.random.normal(key_mix, (GROUP_SIZE * TOKENS_DEV, TOP_K), jnp.float32) * 1.5
    return {
        "dispatched": dispatched.astype(jnp.bfloat16),
        "w_gate": w_gate.astype(jnp.bfloat16),
        "w_up": w_up.astype(jnp.bfloat16),
        "w_down": w_down.astype(jnp.bfloat16),
        "fill_count": filled_count,
        "slot_index": slot_index,
        "expert_id": expert_id,
        "gate_weight": jax.nn.softmax(logits, axis=-1),
    }


def reference(dispatched, w_gate, w_up, w_down, fill_count, slot_index, expert_id, gate_weight):
    group_size = dispatched.shape[0]
    capacity = dispatched.shape[2]
    tokens_dev = slot_index.shape[0] // group_size

    def expert_ffn(operands):
        row_block, gate_w, up_w, down_w, filled = operands
        rows_f32 = row_block.astype(jnp.float32)
        pre_gate = jnp.einsum("scd,df->scf", rows_f32, gate_w.astype(jnp.float32))
        pre_up = jnp.einsum("scd,df->scf", rows_f32, up_w.astype(jnp.float32))
        hidden = (jax.nn.silu(pre_gate) * pre_up).astype(jnp.bfloat16)
        result = jnp.einsum("scf,fd->scd", hidden.astype(jnp.float32), down_w.astype(jnp.float32)).astype(jnp.bfloat16)
        live_mask = jnp.arange(capacity)[None, :] < filled[:, None]
        return jnp.where(live_mask[:, :, None], result, jnp.zeros_like(result))

    expert_out = lax.map(expert_ffn, (jnp.swapaxes(dispatched, 0, 1), w_gate, w_up, w_down, jnp.swapaxes(fill_count, 0, 1)))
    flat_rows = expert_out.reshape(-1, expert_out.shape[-1])
    source = (jnp.arange(slot_index.shape[0]) // tokens_dev)[:, None]
    row_index = (expert_id * group_size + source) * capacity + jnp.maximum(slot_index, 0)
    weight = jnp.where(slot_index >= 0, gate_weight, 0.0)
    combined = jnp.zeros((slot_index.shape[0], flat_rows.shape[1]), jnp.float32)
    for choice in range(slot_index.shape[1]):
        picked = jnp.take(flat_rows, row_index[:, choice], axis=0).astype(jnp.float32)
        combined = combined + weight[:, choice, None] * picked
    return combined.astype(jnp.bfloat16)
```

```python
import functools

import jax
import jax.numpy as jnp
from jax import lax
from jax.experimental import pallas as pl
from jax.experimental.pallas import tpu as pltpu
from jax.sharding import PartitionSpec as P

MESH = pl.DeviceIdType.MESH
BLOCKS_A = ((4, 0), (-3, 0), (4, 1), (-3, 1), (3, 0), (-2, 0), (3, 1), (-2, 1))
BLOCKS_B = (((2, 0), (-1, 0), (2, 1), (-1, 1)), ((1, 0), (0, 0), (1, 1), (0, 1)))
CLASS = {3: 0, -2: 1, 2: 2, -1: 3, 1: 4, 0: 5}
LEAF = 4
TILE = 512


def kernel(zn, disp, wg, wu, wd, fill, slot, eid, gw, out,
           xa, xb, wgb, wub, wdb, hid, lsend, leaf, ysend, ybuf, head, part, meta, scr, sel,
           xa_sem, xb_sem, w_sem, lsend_sem, leaf_sem, ysend_sem, ybuf_sem, psend_sem, part_sem, msend_sem, meta_sem):
    me = lax.axis_index("ep")
    z, k = me // 2, lax.rem(me, 2)
    sigma = 1 - 2 * k
    experts, cap, dim = disp.shape[1:]
    ffn = wg.shape[2]
    tokens, top_k = slot.shape
    per_core = experts * cap
    chunks, _, width = part.shape[1:]
    units = 3 * experts

    def dev(a, rel):
        chip = lax.rem(z + a * sigma + zn, zn) if rel == 0 else lax.rem(z - a * sigma + zn, zn)
        return 2 * chip + (k if rel == 0 else 1 - k)

    def remote(src, dst, send, recv, target):
        return pltpu.make_async_remote_copy(src_ref=src, dst_ref=dst, send_sem=send, recv_sem=recv,
                                            device_id={"ep": target}, device_id_type=MESH)

    def rows_of(core, e):
        return pl.ds(pl.multiple_of(core * per_core + e * cap, cap), cap)

    def rows_meta(cls):
        return pl.ds(2 * top_k * cls, 2 * top_k)

    def xa_copy(e, b):
        return pltpu.make_async_copy(disp.at[dev(*BLOCKS_A[b]), e], xa.at[e, pl.ds(b * cap, cap)], xa_sem.at[e, b])

    def xb_copy(p, e, b):
        return pltpu.make_async_copy(disp.at[dev(*BLOCKS_B[p][b]), e], xb.at[p, e, pl.ds(b * cap, cap)],
                                     xb_sem.at[p, e, b])

    def w_copy(which, u):
        src, dst = ((wg, wgb), (wu, wub), (wd, wdb))[which]
        return pltpu.make_async_copy(src.at[lax.rem(u, experts)], dst.at[lax.rem(u, 2)], w_sem.at[which, lax.rem(u, 2)])

    def start_xa(e):
        for b in range(len(BLOCKS_A)):
            xa_copy(e, b).start()

    def start_xb(p, e):
        for b in range(len(BLOCKS_B[p])):
            xb_copy(p, e, b).start()

    for u in range(2):
        start_xa(u)
        for which in range(3):
            w_copy(which, u).start()

    scr[...] = jnp.zeros_like(scr)
    flat = jnp.where(slot[...] >= 0, eid[...] * cap + slot[...], -1)
    scr[:, 0:top_k] = flat.astype(jnp.float32)
    scr[:, top_k:2 * top_k] = gw[...]
    own = scr[...].T
    meta[...] = jnp.zeros_like(meta)
    meta[rows_meta(CLASS[0])] = own[0:2 * top_k]

    barrier = pltpu.get_barrier_semaphore()
    partners = [(0, 1), (1, 0), (-1, 0), (1, 1), (-1, 1), (2, 0), (-2, 0), (3, 0), (-3, 0)]
    for a, rel in partners:
        pl.semaphore_signal(barrier, inc=1, device_id={"ep": dev(a, rel)}, device_id_type=MESH)
    pl.semaphore_wait(barrier, len(partners))
    meta_to = [(-3, 0), (2, 1), (-2, 2), (1, 3), (-1, 4)]

    def meta_copy(a, cls):
        return remote(meta.at[rows_meta(CLASS[0])], meta.at[rows_meta(cls)], msend_sem.at[cls], meta_sem.at[cls], dev(a, 0))

    for a, cls in meta_to:
        meta_copy(a, cls).start()

    def up_phase(x_ref, e, u, blocks):
        s = lax.rem(u, 2)
        row = lax.broadcasted_iota(jnp.int32, (cap, TILE), 0)

        def tile(n, carry):
            cols = pl.ds(pl.multiple_of(n * TILE, TILE), TILE)
            x = x_ref[...]
            a = jnp.dot(x, wgb[s, :, cols], preferred_element_type=jnp.float32)
            b = jnp.dot(x, wub[s, :, cols], preferred_element_type=jnp.float32)
            h = jax.nn.silu(a) * b
            for i, block in enumerate(blocks):
                live = row < fill[dev(*block), e]
                hid[i * cap:(i + 1) * cap, cols] = jnp.where(live, h[i * cap:(i + 1) * cap], 0.0).astype(jnp.bfloat16)
            return carry

        lax.fori_loop(0, ffn // TILE, tile, 0)

    def down_phase(e, u, blocks, first):
        s = lax.rem(u, 2)
        rows = len(blocks) * cap

        def tile(n, carry):
            cols = pl.ds(pl.multiple_of(n * TILE, TILE), TILE)
            y = jnp.dot(hid[0:rows], wdb[s, :, cols], preferred_element_type=jnp.float32).astype(jnp.bfloat16)
            for i, (a, rel) in enumerate(blocks):
                block = y[i * cap:(i + 1) * cap]
                if first and i < LEAF:
                    lsend[i, e, :, cols] = block
                elif rel == 0:
                    ybuf[CLASS[a], rows_of(0, e), cols] = block
                else:
                    ysend[CLASS[a], e, :, cols] = block
            return carry

        lax.fori_loop(0, dim // TILE, tile, 0)

    def leaf_copy(i, e):
        rel = BLOCKS_A[i][1]
        way = 1 if BLOCKS_A[i][0] > 0 else -1
        return remote(lsend.at[i, e], leaf.at[i % 2, rows_of(rel, e)], lsend_sem.at[i, e], leaf_sem.at[i % 2, rel, e], dev(way, rel))

    def sibling_copy(cls, e):
        return remote(ysend.at[cls, e], ybuf.at[cls, rows_of(1, e)], ysend_sem.at[cls, e], ybuf_sem.at[cls, e], dev(0, 1))

    def unit(x_ref, e, u, blocks, first):
        w_copy(0, u).wait()
        w_copy(1, u).wait()
        up_phase(x_ref, e, u, blocks)

        @pl.when(u + 2 < units)
        def _():
            w_copy(0, u + 2).start()
            w_copy(1, u + 2).start()

        w_copy(2, u).wait()
        down_phase(e, u, blocks, first)

        @pl.when(u + 2 < units)
        def _():
            w_copy(2, u + 2).start()

        for i, (a, rel) in enumerate(blocks):
            if first and i < LEAF:
                leaf_copy(i, e).start()
            elif rel == 1:
                sibling_copy(CLASS[a], e).start()

    def first_unit(e, carry):
        for b in range(len(BLOCKS_A)):
            xa_copy(e, b).wait()

        @pl.when(e + 2 < experts)
        def _():
            start_xa(e + 2)

        @pl.when(e >= experts - 2)
        def _():
            start_xb(0, e - (experts - 2))

        unit(xa.at[e], e, e, BLOCKS_A, True)
        return carry

    lax.fori_loop(0, experts, first_unit, 0)

    for a, cls in meta_to:
        meta_copy(a, cls).wait_recv()
    scr[...] = meta[...].T
    col = lax.broadcasted_iota(jnp.int32, (tokens, 2 * per_core), 1)
    order = lax.rem(col + k * per_core, 2 * per_core)

    def select(where, cls, a_chip):
        chip = lax.rem(z + a_chip * sigma + zn, zn)
        want = (order + chip * (2 * per_core)).astype(jnp.float32)
        weight = jnp.zeros((tokens, 2 * per_core), jnp.float32)
        for j in range(top_k):
            c = 2 * top_k * cls + j
            weight = jnp.where(scr[:, c:c + 1] == want, scr[:, c + top_k:c + top_k + 1], weight)
        for i in range(3):
            piece = weight.astype(jnp.bfloat16)
            sel[where, i * tokens:(i + 1) * tokens] = piece
            weight = weight - piece.astype(jnp.float32)

    def weigh(where, rows_ref, cols):
        rows = rows_ref[:, cols]
        p = jnp.dot(sel[where], rows, preferred_element_type=jnp.float32)
        return p[0:tokens] + p[tokens:2 * tokens] + p[2 * tokens:3 * tokens]

    def part_copy(src, to, c, a):
        return remote(src, part.at[to, c], psend_sem.at[to, c], part_sem.at[to, c], dev(a, 0))

    def wait_sibling(cls):
        for e in range(experts):
            sibling_copy(cls, e).wait_recv()

    def columns(c):
        return pl.ds(pl.multiple_of(c * width, width), width)

    for i, cls in enumerate((0, 1)):
        select(2 * i, cls, -1 if i == 0 else 1)
        select(2 * i + 1, cls, 0)
    for cls in (0, 1):
        wait_sibling(cls)
    for i in range(LEAF):
        for e in range(experts):
            leaf_copy(i, e).wait_recv()

    def second(c, carry):
        for i in range(2):
            head[i, c] = (weigh(2 * i, leaf.at[i], columns(c))
                          + weigh(2 * i + 1, ybuf.at[i], columns(c)))
            part_copy(head.at[i, c], i, c, 1 if i == 0 else -1).start()
        return carry

    lax.fori_loop(0, chunks, second, 0)

    def later_unit(p):
        def body(e, carry):
            for b in range(len(BLOCKS_B[p])):
                xb_copy(p, e, b).wait()
            if p == 0:
                @pl.when(e + 2 < experts)
                def _():
                    start_xb(0, e + 2)

                @pl.when(e >= experts - 2)
                def _():
                    start_xb(1, e - (experts - 2))
            else:
                @pl.when(e + 2 < experts)
                def _():
                    start_xb(1, e + 2)
            unit(xb.at[p, e], e, experts * (p + 1) + e, BLOCKS_B[p], False)
            return carry
        return body

    lax.fori_loop(0, experts, later_unit(0), 0)
    select(0, 2, 0)
    select(1, 3, 0)
    wait_sibling(2)
    wait_sibling(3)

    def third(c, carry):
        for i in range(2):
            mine = weigh(i, ybuf.at[2 + i], columns(c))
            way = 1 if i == 0 else -1
            part_copy(head.at[i, c], i, c, way).wait_recv()
            part[i, c] = part[i, c] + mine
            part_copy(part.at[i, c], 2 + i, c, way).start()
        return carry

    lax.fori_loop(0, chunks, third, 0)

    lax.fori_loop(0, experts, later_unit(1), 0)
    select(0, 4, 0)
    select(1, 5, 0)
    wait_sibling(4)
    wait_sibling(5)

    def fourth(c, carry):
        mine = weigh(0, ybuf.at[4], columns(c))
        part_copy(part.at[0, c], 2, c, 1).wait_recv()
        part[2, c] = part[2, c] + mine
        part_copy(part.at[2, c], 4, c, 1).start()
        return carry

    lax.fori_loop(0, chunks, fourth, 0)

    def last(c, carry):
        mine = weigh(1, ybuf.at[5], columns(c))
        part_copy(part.at[1, c], 3, c, -1).wait_recv()
        mine = mine + part[3, c]
        part_copy(part.at[2, c], 4, c, 1).wait_recv()
        out[:, columns(c)] = (mine + part[4, c]).astype(out.dtype)
        return carry

    lax.fori_loop(0, chunks, last, 0)

    for a, cls in meta_to:
        meta_copy(a, cls).wait_send()

    def sent_rows(e, carry):
        for i in range(LEAF):
            leaf_copy(i, e).wait_send()
        for cls in range(6):
            sibling_copy(cls, e).wait_send()
        return carry

    lax.fori_loop(0, experts, sent_rows, 0)

    def sent_parts(c, carry):
        part_copy(head.at[0, c], 0, c, 1).wait_send()
        part_copy(head.at[1, c], 1, c, -1).wait_send()
        part_copy(part.at[0, c], 2, c, 1).wait_send()
        part_copy(part.at[1, c], 3, c, -1).wait_send()
        part_copy(part.at[2, c], 4, c, 1).wait_send()
        return carry

    lax.fori_loop(0, chunks, sent_parts, 0)


def solution(mesh):
    zn = mesh.shape["ep"] // 2

    def local_step(dispatched, w_gate, w_up, w_down, fill_count, slot_index, expert_id, gate_weight):
        sources, experts, cap, dim = dispatched.shape
        ffn = w_gate.shape[2]
        tokens = slot_index.shape[0]
        bf16, f32 = jnp.bfloat16, jnp.float32
        width = TILE
        chunks = dim // width
        rows_a, rows_b = len(BLOCKS_A) * cap, len(BLOCKS_B[0]) * cap
        any_spec, vmem = pl.BlockSpec(memory_space=pl.ANY), pl.BlockSpec(memory_space=pltpu.VMEM)
        dma = pltpu.SemaphoreType.DMA
        return pl.pallas_call(
            functools.partial(kernel, zn),
            out_shape=jax.ShapeDtypeStruct((tokens, dim), bf16),
            in_specs=[any_spec] * 4 + [pl.BlockSpec(memory_space=pltpu.SMEM)] + [vmem] * 3,
            out_specs=vmem,
            scratch_shapes=[
                pltpu.VMEM((experts, rows_a, dim), bf16),
                pltpu.VMEM((2, experts, rows_b, dim), bf16),
                pltpu.VMEM((2, dim, ffn), bf16),
                pltpu.VMEM((2, dim, ffn), bf16),
                pltpu.VMEM((2, ffn, dim), bf16),
                pltpu.VMEM((rows_a, ffn), bf16),
                pltpu.VMEM((LEAF, experts, cap, dim), bf16),
                pltpu.VMEM((2, 2 * experts * cap, dim), bf16),
                pltpu.VMEM((6, experts, cap, dim), bf16),
                pltpu.VMEM((6, 2 * experts * cap, dim), bf16),
                pltpu.VMEM((2, chunks, tokens, width), f32),
                pltpu.VMEM((5, chunks, tokens, width), f32),
                pltpu.VMEM((128, tokens), f32),
                pltpu.VMEM((128, 128), f32),
                pltpu.VMEM((4, 3 * tokens, 2 * experts * cap), bf16),
                dma((experts, len(BLOCKS_A))),
                dma((2, experts, len(BLOCKS_B[0]))),
                dma((3, 2)),
                dma((LEAF, experts)),
                dma((2, 2, experts)),
                dma((6, experts)),
                dma((6, experts)),
                dma((5, chunks)),
                dma((5, chunks)),
                dma((5,)),
                dma((5,)),
            ],
            compiler_params=pltpu.CompilerParams(
                collective_id=0, has_side_effects=True, vmem_limit_bytes=67043328),
        )(dispatched, w_gate, w_up, w_down, fill_count, slot_index, expert_id, gate_weight)

    token_spec = P(("dp", "ep"))
    in_specs = (P("dp", "ep"), P("ep"), P("ep"), P("ep"), P("dp", "ep"), token_spec, token_spec, token_spec)
    return jax.shard_map(local_step, mesh=mesh, in_specs=in_specs, out_specs=token_spec, check_vma=False)
```

```python
import functools

import jax
import jax.numpy as jnp
from jax import lax
from jax.experimental import pallas as pl
from jax.experimental.pallas import tpu as pltpu
from jax.sharding import PartitionSpec as P

MESH = pl.DeviceIdType.MESH
BLOCKS_L = ((4, 0), (-3, 0), (4, 1), (-3, 1))
BLOCKS_R = ((3, 0), (-2, 0), (3, 1), (-2, 1))
BLOCKS_A = (BLOCKS_L, BLOCKS_R)
BLOCKS_B = (((2, 0), (-1, 0), (2, 1), (-1, 1)), ((1, 0), (0, 0), (1, 1), (0, 1)))
CLASS = {3: 0, -2: 1, 2: 2, -1: 3, 1: 4, 0: 5}
TILE = 512


def kernel(zn, disp, wg, wu, wd, fill_hbm, slot_hbm, eid_hbm, gw_hbm, out,
           xa, xb, wgb, wub, wdb, hid, lsend, leaf, ysend, ybuf, head, part, meta, scr, sel, outv, fill, slot, eid, gw,
           x_sem, gu_sem, d_sem, small_sem, leaf_sem, ybuf_sem, part_sem, meta_sem, send_sem, out_sem):
    me = lax.axis_index("ep")
    z, k = me // 2, lax.rem(me, 2)
    sigma = 1 - 2 * k
    experts, cap, dim = disp.shape[1:]
    ffn = wg.shape[2]
    top_k, tokens = slot.shape
    per_core = experts * cap
    chunks, _, width = part.shape[1:]
    ups = ffn // width
    rows = len(BLOCKS_L) * cap
    lsend_sem, ysend_sem, head_sem, psend_sem, msend_sem = (send_sem.at[i] for i in range(5))

    def dev(a, rel):
        chip = lax.rem(z + a * sigma + zn, zn) if rel == 0 else lax.rem(z - a * sigma + zn, zn)
        return 2 * chip + (k if rel == 0 else 1 - k)

    def remote(src, dst, send, recv, target):
        return pltpu.make_async_remote_copy(src_ref=src, dst_ref=dst, send_sem=send, recv_sem=recv,
                                            device_id={"ep": target}, device_id_type=MESH)

    def rows_of(core, e):
        return pl.ds(pl.multiple_of(core * per_core + e * cap, cap), cap)

    def rows_meta(cls):
        return pl.ds(2 * top_k * cls, 2 * top_k)

    def columns(c):
        return pl.ds(pl.multiple_of(c * width, width), width)

    def x_copy(h, e, b):
        x, blocks = (xa, BLOCKS_A[h]) if h < 2 else (xb, BLOCKS_B[h - 2])
        return pltpu.make_async_copy(disp.at[dev(*blocks[b]), e], x.at[h % 2, e, pl.ds(b * cap, cap)], x_sem.at[h, e])

    def gu_copy(which, e, n):
        src, dst = ((wg, wgb), (wu, wub))[which]
        return pltpu.make_async_copy(src.at[e, :, columns(n)], dst.at[lax.rem(e, 2), :, columns(n)],
                                     gu_sem.at[which, lax.rem(e, 2), n])

    def d_copy(e, n):
        return pltpu.make_async_copy(wd.at[e, :, columns(n)], wdb.at[lax.rem(e, 2), :, columns(n)], d_sem.at[lax.rem(e, 2), n])

    def start_gu(e):
        for n in range(ups):
            for which in range(2):
                gu_copy(which, e, n).start()

    def start_d(e):
        for n in range(chunks):
            d_copy(e, n).start()

    def start_x(h, e):
        for b in range(len(BLOCKS_L)):
            x_copy(h, e, b).start()

    def arrived(ref, sem):
        pltpu.make_async_copy(ref, ref, sem).wait()

    def wait_x(h, e):
        arrived((xa if h < 2 else xb).at[h % 2, e], x_sem.at[h, e])

    small = [pltpu.make_async_copy(src, dst, small_sem.at[i]) for i, (src, dst) in enumerate(
        ((fill_hbm, fill), (slot_hbm, slot), (eid_hbm, eid), (gw_hbm, gw)))]
    start_x(0, 0)
    start_gu(0)
    for copy in small:
        copy.start()
    start_d(0)
    for copy in small:
        copy.wait()

    flat = jnp.where(slot[...] >= 0, eid[...] * cap + slot[...], -1)
    meta[...] = jnp.zeros_like(meta)
    meta[2 * top_k * CLASS[0]:2 * top_k * CLASS[0] + top_k] = flat.astype(jnp.float32)
    meta[2 * top_k * CLASS[0] + top_k:2 * top_k * (CLASS[0] + 1)] = gw[...]

    barrier = pltpu.get_barrier_semaphore()
    partners = [(0, 1), (1, 0), (-1, 0), (1, 1), (-1, 1), (2, 0), (-2, 0), (3, 0), (-3, 0)]
    for a, rel in partners:
        pl.semaphore_signal(barrier, inc=1, device_id={"ep": dev(a, rel)}, device_id_type=MESH)

    def up_phase(x_ref, e, blocks, wait):
        s = lax.rem(e, 2)
        row = lax.broadcasted_iota(jnp.int32, (cap, width), 0)

        def tile(n, carry):
            cols = columns(n)
            if wait:
                for which in range(2):
                    gu_copy(which, e, n).wait()
            x = x_ref[...]
            a = jnp.dot(x, wgb[s, :, cols], preferred_element_type=jnp.float32)
            b = jnp.dot(x, wub[s, :, cols], preferred_element_type=jnp.float32)
            h = jax.nn.silu(a) * b
            for i, block in enumerate(blocks):
                live = row < fill[e, dev(*block)]
                hid[i * cap:(i + 1) * cap, cols] = jnp.where(live, h[i * cap:(i + 1) * cap], 0.0).astype(jnp.bfloat16)
            return carry

        lax.fori_loop(0, ups, tile, 0)

    def leaf_copy(i, e, c):
        a, rel = BLOCKS_L[i]
        return remote(lsend.at[i, e, c], leaf.at[i % 2, c, rows_of(rel, e)], lsend_sem,
                      leaf_sem.at[i % 2, c], dev(1 if a > 0 else -1, rel))

    def sibling_copy(cls, e):
        return remote(ysend.at[cls, e], ybuf.at[cls, :, rows_of(1, e)], ysend_sem, ybuf_sem.at[cls], dev(0, 1))

    def down_phase(e, blocks, wait):
        s = lax.rem(e, 2)
        leaves = blocks is BLOCKS_L

        def tile(n, carry):
            if wait:
                d_copy(e, n).wait()
            y = jnp.dot(hid[...], wdb[s, :, columns(n)], preferred_element_type=jnp.float32).astype(jnp.bfloat16)
            for i, (a, rel) in enumerate(blocks):
                block = y[i * cap:(i + 1) * cap]
                if leaves:
                    lsend[i, e, n] = block
                elif rel == 0:
                    ybuf[CLASS[a], n, rows_of(0, e)] = block
                else:
                    ysend[CLASS[a], e, n] = block
            if leaves:
                for i in range(len(blocks)):
                    leaf_copy(i, e, n).start()
            return carry

        lax.fori_loop(0, chunks, tile, 0)
        if not leaves:
            for a, rel in blocks:
                if rel == 1:
                    sibling_copy(CLASS[a], e).start()

    meta_to = [(-3, 0), (2, 1), (-2, 2), (1, 3), (-1, 4)]

    def meta_copy(a, cls):
        return remote(meta.at[rows_meta(CLASS[0])], meta.at[rows_meta(cls)], msend_sem, meta_sem.at[0], dev(a, 0))

    def leaf_unit(e, carry):
        wait_x(0, e)
        up_phase(xa.at[0, e], e, BLOCKS_L, True)
        down_phase(e, BLOCKS_L, True)
        return carry

    def rest_unit(e, carry, load):
        wait_x(1, e)
        up_phase(xa.at[1, e], e, BLOCKS_R, False)
        if load:
            start_gu(e + 2)
        down_phase(e, BLOCKS_R, False)
        if load:
            start_d(e + 2)
        return carry

    wait_x(0, 0)
    up_phase(xa.at[0, 0], 0, BLOCKS_L, True)
    start_x(0, 1)
    start_gu(1)
    start_d(1)
    for e in range(2):
        start_x(1, e)
    pl.semaphore_wait(barrier, len(partners))
    for a, cls in meta_to:
        meta_copy(a, cls).start()
    down_phase(0, BLOCKS_L, True)
    leaf_unit(1, 0)
    for e in range(2, experts):
        start_x(0, e)
        start_x(1, e)
    lax.fori_loop(0, 2, functools.partial(rest_unit, load=True), 0)
    for e in range(experts):
        start_x(2, e)
    lax.fori_loop(2, experts, leaf_unit, 0)

    arrived(meta.at[pl.ds(0, 2 * top_k * len(meta_to))], meta_sem.at[0])
    scr[...] = meta[...].T
    col = lax.broadcasted_iota(jnp.int32, (tokens, 2 * per_core), 1)
    order = lax.rem(col + k * per_core, 2 * per_core)

    def select(where, cls, a_chip):
        chip = lax.rem(z + a_chip * sigma + zn, zn)
        want = (order + chip * (2 * per_core)).astype(jnp.float32)
        weight = jnp.zeros((tokens, 2 * per_core), jnp.float32)
        for j in range(top_k):
            c = 2 * top_k * cls + j
            weight = jnp.where(scr[:, c:c + 1] == want, scr[:, c + top_k:c + top_k + 1], weight)
        for i in range(3):
            piece = weight.astype(jnp.bfloat16)
            sel[where, i * tokens:(i + 1) * tokens] = piece
            weight = weight - piece.astype(jnp.float32)

    def weigh(where, rows_ref):
        p = jnp.dot(sel[where], rows_ref[...], preferred_element_type=jnp.float32)
        return p[0:tokens] + p[tokens:2 * tokens] + p[2 * tokens:3 * tokens]

    def part_copy(src, to, c, a):
        return remote(src, part.at[to, c], head_sem if to < 2 else psend_sem, part_sem.at[to, c], dev(a, 0))

    def wait_part(to, c):
        arrived(part.at[to, c], part_sem.at[to, c])

    def wait_sibling(cls):
        arrived(ybuf.at[cls, :, pl.ds(per_core, per_core)], ybuf_sem.at[cls])

    for cls in (0, 1):
        select(cls, cls, 0)
        select(6 + cls, cls, -1 if cls == 0 else 1)
    lax.fori_loop(2, experts, functools.partial(rest_unit, load=False), 0)

    for cls in (0, 1):
        wait_sibling(cls)

    def second(c, carry):
        for i in range(2):
            mine = weigh(i, ybuf.at[i, c])
            arrived(leaf.at[i, c], leaf_sem.at[i, c])
            head[i, c] = mine + weigh(6 + i, leaf.at[i, c])
            part_copy(head.at[i, c], i, c, 1 if i == 0 else -1).start()
        return carry

    lax.fori_loop(0, chunks, second, 0)

    def later_unit(p, half):
        def body(q, carry):
            e = q + 2 * ((p + half + 1) % 2)
            wait_x(2 + p, e)
            up_phase(xb.at[p, e], e, BLOCKS_B[p], half == 1)
            if half == 0:
                start_gu(lax.rem(e + 2, experts))
            down_phase(e, BLOCKS_B[p], half == 1)
            if half == 0:
                start_d(lax.rem(e + 2, experts))
            return carry
        return body

    def later_pass(p):
        for half in range(2):
            lax.fori_loop(0, 2, later_unit(p, half), 0)

    for cls in range(2, 6):
        select(cls, cls, 0)
    for e in range(experts):
        start_x(3, e)
    later_pass(0)
    wait_sibling(2)
    wait_sibling(3)

    def third(c, carry):
        for i in range(2):
            mine = weigh(2 + i, ybuf.at[2 + i, c])
            way = 1 if i == 0 else -1
            wait_part(i, c)
            part[i, c] = part[i, c] + mine
            part_copy(part.at[i, c], 2 + i, c, way).start()
        return carry

    lax.fori_loop(0, chunks, third, 0)

    later_pass(1)
    wait_sibling(4)
    wait_sibling(5)

    def fourth(c, carry):
        mine = weigh(4, ybuf.at[4, c])
        wait_part(2, c)
        part[2, c] = part[2, c] + mine
        part_copy(part.at[2, c], 4, c, 1).start()
        return carry

    lax.fori_loop(0, chunks, fourth, 0)

    def out_copy(c):
        return pltpu.make_async_copy(outv.at[c], out.at[:, columns(c)], out_sem.at[0])

    def last(c, carry):
        mine = weigh(5, ybuf.at[5, c])
        wait_part(3, c)
        mine = mine + part[3, c]
        wait_part(4, c)
        outv[c] = (mine + part[4, c]).astype(out.dtype)
        out_copy(c).start()
        return carry

    lax.fori_loop(0, chunks, last, 0)

    arrived(outv, out_sem.at[0])
    arrived(meta.at[pl.ds(0, 2 * top_k * len(meta_to))], msend_sem)
    arrived(lsend, lsend_sem)
    arrived(ysend, ysend_sem)
    arrived(head, head_sem)
    arrived(part.at[pl.ds(0, 3)], psend_sem)


def solution(mesh):
    zn = mesh.shape["ep"] // 2

    def local_step(dispatched, w_gate, w_up, w_down, fill_count, slot_index, expert_id, gate_weight):
        sources, experts, cap, dim = dispatched.shape
        ffn = w_gate.shape[2]
        tokens = slot_index.shape[0]
        bf16, f32 = jnp.bfloat16, jnp.float32
        width = TILE
        chunks = dim // width
        blocks = len(BLOCKS_L)
        rows = blocks * cap
        any_spec = pl.BlockSpec(memory_space=pl.ANY)
        dma = pltpu.SemaphoreType.DMA
        return pl.pallas_call(
            functools.partial(kernel, zn),
            out_shape=jax.ShapeDtypeStruct((tokens, dim), bf16),
            in_specs=[any_spec] * 8,
            out_specs=any_spec,
            scratch_shapes=[
                pltpu.VMEM((2, experts, rows, dim), bf16),
                pltpu.VMEM((2, experts, rows, dim), bf16),
                pltpu.VMEM((2, dim, ffn), bf16),
                pltpu.VMEM((2, dim, ffn), bf16),
                pltpu.VMEM((2, ffn, dim), bf16),
                pltpu.VMEM((rows, ffn), bf16),
                pltpu.VMEM((blocks, experts, chunks, cap, width), bf16),
                pltpu.VMEM((2, chunks, 2 * experts * cap, width), bf16),
                pltpu.VMEM((6, experts, chunks, cap, width), bf16),
                pltpu.VMEM((6, chunks, 2 * experts * cap, width), bf16),
                pltpu.VMEM((2, chunks, tokens, width), f32),
                pltpu.VMEM((5, chunks, tokens, width), f32),
                pltpu.VMEM((128, tokens), f32),
                pltpu.VMEM((128, 128), f32),
                pltpu.VMEM((8, 3 * tokens, 2 * experts * cap), bf16),
                pltpu.VMEM((chunks, tokens, width), bf16),
                pltpu.SMEM((experts, sources), jnp.int32),
                pltpu.VMEM(slot_index.shape[::-1], jnp.int32),
                pltpu.VMEM(expert_id.shape[::-1], jnp.int32),
                pltpu.VMEM(gate_weight.shape[::-1], f32),
                dma((4, experts)),
                dma((2, 2, ffn // width)),
                dma((2, chunks)),
                dma((4,)),
                dma((2, chunks)),
                dma((6,)),
                dma((5, chunks)),
                dma((1,)),
                dma((5,)),
                dma((1,)),
            ],
            compiler_params=pltpu.CompilerParams(
                collective_id=0, has_side_effects=True, vmem_limit_bytes=67043328),
        )(dispatched, w_gate, w_up, w_down, fill_count.T, slot_index.T, expert_id.T, gate_weight.T)

    token_spec = P(("dp", "ep"))
    in_specs = (P("dp", "ep"), P("ep"), P("ep"), P("ep"), P("dp", "ep"), token_spec, token_spec, token_spec)
    return jax.shard_map(local_step, mesh=mesh, in_specs=in_specs, out_specs=token_spec, check_vma=False)
```

```python
import functools

import jax
import jax.numpy as jnp
from jax import lax
from jax.experimental import pallas as pl
from jax.experimental.pallas import tpu as pltpu
from jax.sharding import PartitionSpec as P

MESH = pl.DeviceIdType.MESH
BLOCKS_L = ((4, 0), (-3, 0), (4, 1), (-3, 1))
BLOCKS_R = ((3, 0), (-2, 0), (3, 1), (-2, 1))
BLOCKS_A = (BLOCKS_L, BLOCKS_R)
BLOCKS_B = (((2, 0), (-1, 0), (2, 1), (-1, 1)), ((1, 0), (0, 0), (1, 1), (0, 1)))
CLASS = {3: 0, -2: 1, 2: 2, -1: 3, 1: 4, 0: 5}
TILE = 512
UP_TILE = 512


def kernel(zn, disp, wg, wu, wd, fill_hbm, slot_hbm, eid_hbm, gw_hbm, out,
           xa, xb, wgb, wub, wdb, hid, lsend, leaf, ysend, ybuf, head, part, meta, scr, sel, outv, fill, slot, eid, gw,
           x_sem, gu_sem, d_sem, small_sem, leaf_sem, ybuf_sem, part_sem, meta_sem, send_sem, out_sem):
    me = lax.axis_index("ep")
    z, k = me // 2, lax.rem(me, 2)
    sigma = 1 - 2 * k
    experts, cap, dim = disp.shape[1:]
    ffn = wg.shape[2]
    top_k, tokens = slot.shape
    per_core = experts * cap
    chunks, _, width = part.shape[1:]
    ups = ffn // UP_TILE
    rows = len(BLOCKS_L) * cap
    lsend_sem, ysend_sem, head_sem, psend_sem, msend_sem = (send_sem.at[i] for i in range(5))

    def dev(a, rel):
        chip = lax.rem(z + a * sigma + zn, zn) if rel == 0 else lax.rem(z - a * sigma + zn, zn)
        return 2 * chip + (k if rel == 0 else 1 - k)

    def remote(src, dst, send, recv, target):
        return pltpu.make_async_remote_copy(src_ref=src, dst_ref=dst, send_sem=send, recv_sem=recv,
                                            device_id={"ep": target}, device_id_type=MESH)

    def rows_of(core, e):
        return pl.ds(pl.multiple_of(core * per_core + e * cap, cap), cap)

    def rows_meta(cls):
        return pl.ds(2 * top_k * cls, 2 * top_k)

    def columns(c, wide=width):
        return pl.ds(pl.multiple_of(c * wide, wide), wide)

    def x_copy(h, e, b):
        x, blocks = (xa, BLOCKS_A[h]) if h < 2 else (xb, BLOCKS_B[h - 2])
        return pltpu.make_async_copy(disp.at[dev(*blocks[b]), e], x.at[h % 2, e, pl.ds(b * cap, cap)], x_sem.at[h, e if h < 2 else 0])

    def gu_copy(which, e, n):
        src, dst = ((wg, wgb), (wu, wub))[which]
        return pltpu.make_async_copy(src.at[e, :, columns(n, UP_TILE)], dst.at[lax.rem(e, 2), :, columns(n, UP_TILE)],
                                     gu_sem.at[which, lax.rem(e, 2), n])

    def d_copy(e, n):
        return pltpu.make_async_copy(wd.at[e, :, columns(n)], wdb.at[lax.rem(e, 2), :, columns(n)], d_sem.at[lax.rem(e, 2), n])

    def start_gu(e):
        for n in range(ups):
            for which in range(2):
                gu_copy(which, e, n).start()

    def start_d(e):
        for n in range(chunks):
            d_copy(e, n).start()

    def start_x(h, e):
        for b in range(len(BLOCKS_L)):
            x_copy(h, e, b).start()

    def arrived(ref, sem):
        pltpu.make_async_copy(ref, ref, sem).wait()

    def wait_x(h, e):
        arrived(xa.at[h, e], x_sem.at[h, e])

    small = [pltpu.make_async_copy(src, dst, small_sem.at[i]) for i, (src, dst) in enumerate(
        ((fill_hbm, fill), (slot_hbm, slot), (eid_hbm, eid), (gw_hbm, gw)))]
    start_x(0, 0)
    start_gu(0)
    for copy in small:
        copy.start()
    start_d(0)
    for copy in small:
        copy.wait()

    flat = jnp.where(slot[...] >= 0, eid[...] * cap + slot[...], -1)
    meta[...] = jnp.zeros_like(meta)
    meta[2 * top_k * CLASS[0]:2 * top_k * CLASS[0] + top_k] = flat.astype(jnp.float32)
    meta[2 * top_k * CLASS[0] + top_k:2 * top_k * (CLASS[0] + 1)] = gw[...]

    barrier = pltpu.get_barrier_semaphore()
    partners = [(0, 1), (1, 0), (-1, 0), (1, 1), (-1, 1), (2, 0), (-2, 0), (3, 0), (-3, 0)]
    for a, rel in partners:
        pl.semaphore_signal(barrier, inc=1, device_id={"ep": dev(a, rel)}, device_id_type=MESH)

    def up_phase(x_ref, e, blocks, wait):
        s = lax.rem(e, 2)
        row = lax.broadcasted_iota(jnp.int32, (cap, UP_TILE), 0)

        def tile(n, carry):
            cols = columns(n, UP_TILE)
            if wait:
                for which in range(2):
                    gu_copy(which, e, n).wait()
            x = x_ref[...]
            a = jnp.dot(x, wgb[s, :, cols], preferred_element_type=jnp.float32)
            b = jnp.dot(x, wub[s, :, cols], preferred_element_type=jnp.float32)
            h = jax.nn.silu(a) * b
            for i, block in enumerate(blocks):
                live = row < fill[e, dev(*block)]
                hid[i * cap:(i + 1) * cap, cols] = jnp.where(live, h[i * cap:(i + 1) * cap], 0.0).astype(jnp.bfloat16)
            return carry

        lax.fori_loop(0, ups, tile, 0, unroll=True)

    def leaf_copy(i, e, c):
        a, rel = BLOCKS_L[i]
        return remote(lsend.at[i, e, c], leaf.at[i % 2, c, rows_of(rel, e)], lsend_sem,
                      leaf_sem.at[i % 2, c], dev(1 if a > 0 else -1, rel))

    def sibling_copy(cls, e):
        return remote(ysend.at[cls, e], ybuf.at[cls, :, rows_of(1, e)], ysend_sem, ybuf_sem.at[cls], dev(0, 1))

    def down_phase(e, blocks, wait):
        s = lax.rem(e, 2)
        leaves = blocks is BLOCKS_L

        def tile(n, carry):
            if wait:
                d_copy(e, n).wait()
            y = jnp.dot(hid[...], wdb[s, :, columns(n)], preferred_element_type=jnp.float32).astype(jnp.bfloat16)
            for i, (a, rel) in enumerate(blocks):
                block = y[i * cap:(i + 1) * cap]
                if leaves:
                    lsend[i, e, n] = block
                elif rel == 0:
                    ybuf[CLASS[a], n, rows_of(0, e)] = block
                else:
                    ysend[CLASS[a], e, n] = block
            if leaves:
                for i in range(len(blocks)):
                    leaf_copy(i, e, n).start()
            return carry

        lax.fori_loop(0, chunks, tile, 0, unroll=True)
        if not leaves:
            for a, rel in blocks:
                if rel == 1:
                    sibling_copy(CLASS[a], e).start()

    meta_to = [(-3, 0), (2, 1), (-2, 2), (1, 3), (-1, 4)]

    def meta_copy(a, cls):
        return remote(meta.at[rows_meta(CLASS[0])], meta.at[rows_meta(cls)], msend_sem, meta_sem.at[0], dev(a, 0))

    def leaf_unit(e, carry):
        wait_x(0, e)
        up_phase(xa.at[0, e], e, BLOCKS_L, True)
        down_phase(e, BLOCKS_L, True)
        return carry

    def rest_unit(e, carry, load):
        wait_x(1, e)
        up_phase(xa.at[1, e], e, BLOCKS_R, False)
        if load:
            start_gu(e + 2)
        down_phase(e, BLOCKS_R, False)
        if load:
            start_d(e + 2)
        return carry

    wait_x(0, 0)
    up_phase(xa.at[0, 0], 0, BLOCKS_L, True)
    start_x(0, 1)
    start_gu(1)
    start_d(1)
    for e in range(2):
        start_x(1, e)
    pl.semaphore_wait(barrier, len(partners))
    for a, cls in meta_to:
        meta_copy(a, cls).start()
    down_phase(0, BLOCKS_L, True)
    leaf_unit(1, 0)
    for e in range(2, experts):
        start_x(0, e)
        start_x(1, e)
    lax.fori_loop(0, 2, functools.partial(rest_unit, load=True), 0)
    for e in range(experts):
        start_x(2, e)

    arrived(meta.at[pl.ds(0, 2 * top_k * len(meta_to))], meta_sem.at[0])
    scr[...] = meta[...].T
    col = lax.broadcasted_iota(jnp.int32, (tokens, 2 * per_core), 1)
    order = lax.rem(col + k * per_core, 2 * per_core)

    def select(where, cls, a_chip):
        chip = lax.rem(z + a_chip * sigma + zn, zn)
        want = (order + chip * (2 * per_core)).astype(jnp.float32)
        weight = jnp.zeros((tokens, 2 * per_core), jnp.float32)
        for j in range(top_k):
            c = 2 * top_k * cls + j
            weight = jnp.where(scr[:, c:c + 1] == want, scr[:, c + top_k:c + top_k + 1], weight)
        for i in range(3):
            piece = weight.astype(jnp.bfloat16)
            sel[where, i * tokens:(i + 1) * tokens] = piece
            weight = weight - piece.astype(jnp.float32)

    for cls in (0, 1):
        select(cls, cls, 0)
        select(6 + cls, cls, -1 if cls == 0 else 1)

    lax.fori_loop(2, experts, leaf_unit, 0)


    def weigh(where, rows_ref):
        p = jnp.dot(sel[where], rows_ref[...], preferred_element_type=jnp.float32)
        return p[0:tokens] + p[tokens:2 * tokens] + p[2 * tokens:3 * tokens]

    def part_copy(src, to, c, a):
        return remote(src, part.at[to, c], head_sem if to < 2 else psend_sem, part_sem.at[to, c], dev(a, 0))

    def wait_part(to, c):
        arrived(part.at[to, c], part_sem.at[to, c])

    def wait_sibling(cls):
        arrived(ybuf.at[cls, :, pl.ds(per_core, per_core)], ybuf_sem.at[cls])

    lax.fori_loop(2, experts, functools.partial(rest_unit, load=False), 0)

    for cls in (0, 1):
        wait_sibling(cls)

    def second(c, carry):
        for i in range(2):
            mine = weigh(i, ybuf.at[i, c])
            arrived(leaf.at[i, c], leaf_sem.at[i, c])
            head[i, c] = mine + weigh(6 + i, leaf.at[i, c])
            part_copy(head.at[i, c], i, c, 1 if i == 0 else -1).start()
        return carry

    lax.fori_loop(0, chunks, second, 0)

    def later_unit(p, half):
        def body(q, carry):
            e = q + 2 * ((p + half + 1) % 2)
            up_phase(xb.at[p, e], e, BLOCKS_B[p], half == 1)
            if half == 0:
                start_gu(lax.rem(e + 2, experts))
            down_phase(e, BLOCKS_B[p], half == 1)
            if half == 0:
                start_d(lax.rem(e + 2, experts))
            return carry
        return body

    def later_pass(p):
        arrived(xb.at[p], x_sem.at[2 + p, 0])
        for half in range(2):
            lax.fori_loop(0, 2, later_unit(p, half), 0)

    for cls in range(2, 6):
        select(cls, cls, 0)
    for e in range(experts):
        start_x(3, e)
    later_pass(0)
    wait_sibling(2)
    wait_sibling(3)

    def third(c, carry):
        for i in range(2):
            mine = weigh(2 + i, ybuf.at[2 + i, c])
            way = 1 if i == 0 else -1
            wait_part(i, c)
            part[i, c] = part[i, c] + mine
            part_copy(part.at[i, c], 2 + i, c, way).start()
        return carry

    lax.fori_loop(0, chunks, third, 0)

    later_pass(1)
    wait_sibling(4)
    wait_sibling(5)

    def fourth(c, carry):
        mine = weigh(4, ybuf.at[4, c])
        wait_part(2, c)
        part[2, c] = part[2, c] + mine
        part_copy(part.at[2, c], 4, c, 1).start()
        return carry

    lax.fori_loop(0, chunks, fourth, 0)

    def out_copy(c):
        return pltpu.make_async_copy(outv.at[c], out.at[:, columns(c)], out_sem.at[0])

    def last(c, carry):
        mine = weigh(5, ybuf.at[5, c])
        wait_part(3, c)
        mine = mine + part[3, c]
        wait_part(4, c)
        outv[c] = (mine + part[4, c]).astype(out.dtype)
        out_copy(c).start()
        return carry

    lax.fori_loop(0, chunks, last, 0)

    arrived(outv, out_sem.at[0])
    arrived(meta.at[pl.ds(0, 2 * top_k * len(meta_to))], msend_sem)
    arrived(lsend, lsend_sem)
    arrived(ysend, ysend_sem)
    arrived(head, head_sem)
    arrived(part.at[pl.ds(0, 3)], psend_sem)


def solution(mesh):
    zn = mesh.shape["ep"] // 2

    def local_step(dispatched, w_gate, w_up, w_down, fill_count, slot_index, expert_id, gate_weight):
        sources, experts, cap, dim = dispatched.shape
        ffn = w_gate.shape[2]
        tokens = slot_index.shape[0]
        bf16, f32 = jnp.bfloat16, jnp.float32
        width = TILE
        chunks = dim // width
        blocks = len(BLOCKS_L)
        rows = blocks * cap
        any_spec = pl.BlockSpec(memory_space=pl.ANY)
        dma = pltpu.SemaphoreType.DMA
        return pl.pallas_call(
            functools.partial(kernel, zn),
            out_shape=jax.ShapeDtypeStruct((tokens, dim), bf16),
            in_specs=[any_spec] * 8,
            out_specs=any_spec,
            scratch_shapes=[
                pltpu.VMEM((2, experts, rows, dim), bf16),
                pltpu.VMEM((2, experts, rows, dim), bf16),
                pltpu.VMEM((2, dim, ffn), bf16),
                pltpu.VMEM((2, dim, ffn), bf16),
                pltpu.VMEM((2, ffn, dim), bf16),
                pltpu.VMEM((rows, ffn), bf16),
                pltpu.VMEM((blocks, experts, chunks, cap, width), bf16),
                pltpu.VMEM((2, chunks, 2 * experts * cap, width), bf16),
                pltpu.VMEM((6, experts, chunks, cap, width), bf16),
                pltpu.VMEM((6, chunks, 2 * experts * cap, width), bf16),
                pltpu.VMEM((2, chunks, tokens, width), f32),
                pltpu.VMEM((5, chunks, tokens, width), f32),
                pltpu.VMEM((128, tokens), f32),
                pltpu.VMEM((128, 128), f32),
                pltpu.VMEM((8, 3 * tokens, 2 * experts * cap), bf16),
                pltpu.VMEM((chunks, tokens, width), bf16),
                pltpu.SMEM((experts, sources), jnp.int32),
                pltpu.VMEM(slot_index.shape[::-1], jnp.int32),
                pltpu.VMEM(expert_id.shape[::-1], jnp.int32),
                pltpu.VMEM(gate_weight.shape[::-1], f32),
                dma((4, experts)),
                dma((2, 2, ffn // UP_TILE)),
                dma((2, chunks)),
                dma((4,)),
                dma((2, chunks)),
                dma((6,)),
                dma((5, chunks)),
                dma((1,)),
                dma((5,)),
                dma((1,)),
            ],
            compiler_params=pltpu.CompilerParams(
                collective_id=0, has_side_effects=True, vmem_limit_bytes=67043328),
        )(dispatched, w_gate, w_up, w_down, fill_count.T, slot_index.T, expert_id.T, gate_weight.T)

    token_spec = P(("dp", "ep"))
    in_specs = (P("dp", "ep"), P("ep"), P("ep"), P("ep"), P("dp", "ep"), token_spec, token_spec, token_spec)
    return jax.shard_map(local_step, mesh=mesh, in_specs=in_specs, out_specs=token_spec, check_vma=False)
```

```python
import functools

import jax
import jax.numpy as jnp
from jax import lax
from jax.experimental import pallas as pl
from jax.experimental.pallas import tpu as pltpu
from jax.sharding import PartitionSpec as P

MESH = pl.DeviceIdType.MESH
BLOCKS_L = ((4, 0), (-3, 0), (4, 1), (-3, 1))
BLOCKS_R = ((3, 0), (-2, 0), (3, 1), (-2, 1))
BLOCKS_A = (BLOCKS_L, BLOCKS_R)
BLOCKS_B = (((2, 0), (-1, 0), (2, 1), (-1, 1)), ((1, 0), (0, 0), (1, 1), (0, 1)))
CLASS = {3: 0, -2: 1, 2: 2, -1: 3, 1: 4, 0: 5}
TILE = 512
UP_TILE = 512


def kernel(zn, disp, wg, wu, wd, fill_hbm, slot_hbm, eid_hbm, gw_hbm, out,
           xa, xb, wgb, wub, wdb, hid, lsend, leaf, ysend, ybuf, head, part, meta, scr, sel, outv, fill, slot, eid, gw,
           x_sem, gu_sem, d_sem, small_sem, leaf_sem, ybuf_sem, part_sem, meta_sem, send_sem, out_sem):
    me = lax.axis_index("ep")
    z, k = me // 2, lax.rem(me, 2)
    sigma = 1 - 2 * k
    experts, cap, dim = disp.shape[1:]
    ffn = wg.shape[2]
    top_k, tokens = slot.shape
    per_core = experts * cap
    chunks, _, width = part.shape[1:]
    ups = ffn // UP_TILE
    rows = len(BLOCKS_L) * cap
    lsend_sem, ysend_sem, head_sem, psend_sem, msend_sem = (send_sem.at[i] for i in range(5))

    def dev(a, rel):
        chip = lax.rem(z + a * sigma + zn, zn) if rel == 0 else lax.rem(z - a * sigma + zn, zn)
        return 2 * chip + (k if rel == 0 else 1 - k)

    def remote(src, dst, send, recv, target):
        return pltpu.make_async_remote_copy(src_ref=src, dst_ref=dst, send_sem=send, recv_sem=recv,
                                            device_id={"ep": target}, device_id_type=MESH)

    def rows_of(core, e):
        return pl.ds(pl.multiple_of(core * per_core + e * cap, cap), cap)

    def rows_meta(cls):
        return pl.ds(2 * top_k * cls, 2 * top_k)

    def columns(c, wide=width):
        if isinstance(c, int):
            return pl.ds(c * wide, wide)
        return pl.ds(pl.multiple_of(c * wide, wide), wide)

    def x_copy(h, e, b):
        x, blocks = (xa, BLOCKS_A[h]) if h < 2 else (xb, BLOCKS_B[h - 2])
        return pltpu.make_async_copy(disp.at[dev(*blocks[b]), e], x.at[h % 2, e, pl.ds(b * cap, cap)], x_sem.at[h, e if h < 2 else 0])

    def gu_copy(which, e, n):
        src, dst = ((wg, wgb), (wu, wub))[which]
        return pltpu.make_async_copy(src.at[e, :, columns(n, UP_TILE)], dst.at[lax.rem(e, 2), :, columns(n, UP_TILE)],
                                     gu_sem.at[which, lax.rem(e, 2), n])

    def d_copy(e, n):
        return pltpu.make_async_copy(wd.at[e, :, columns(n)], wdb.at[lax.rem(e, 2), :, columns(n)], d_sem.at[lax.rem(e, 2), n])

    def start_gu(e, tiles=None):
        for n in range(ups) if tiles is None else tiles:
            for which in range(2):
                gu_copy(which, e, n).start()

    def start_d(e):
        for n in range(chunks):
            d_copy(e, n).start()

    def start_x(h, e):
        for b in range(len(BLOCKS_L)):
            x_copy(h, e, b).start()

    def arrived(ref, sem):
        pltpu.make_async_copy(ref, ref, sem).wait()

    def wait_x(h, e):
        arrived(xa.at[h, e], x_sem.at[h, e])

    small = [pltpu.make_async_copy(src, dst, small_sem.at[i]) for i, (src, dst) in enumerate(
        ((fill_hbm, fill), (slot_hbm, slot), (eid_hbm, eid), (gw_hbm, gw)))]
    start_x(0, 0)
    start_gu(0, range(1))
    for copy in small:
        copy.start()
    for copy in small:
        copy.wait()
    start_gu(0, range(1, ups))

    flat = jnp.where(slot[...] >= 0, eid[...] * cap + slot[...], -1)
    meta[...] = jnp.zeros_like(meta)
    meta[2 * top_k * CLASS[0]:2 * top_k * CLASS[0] + top_k] = flat.astype(jnp.float32)
    meta[2 * top_k * CLASS[0] + top_k:2 * top_k * (CLASS[0] + 1)] = gw[...]

    barrier = pltpu.get_barrier_semaphore()
    partners = [(0, 1), (1, 0), (-1, 0), (1, 1), (-1, 1), (2, 0), (-2, 0), (3, 0), (-3, 0)]
    for a, rel in partners:
        pl.semaphore_signal(barrier, inc=1, device_id={"ep": dev(a, rel)}, device_id_type=MESH)

    def up_phase(x_ref, e, blocks, wait, after=None):
        s = lax.rem(e, 2)
        row = lax.broadcasted_iota(jnp.int32, (cap, UP_TILE), 0)

        for n in range(ups):
            cols = columns(n, UP_TILE)
            if wait:
                for which in range(2):
                    gu_copy(which, e, n).wait()
            if after is not None and n == 0:
                after()
            x = x_ref[...]
            a = jnp.dot(x, wgb[s, :, cols], preferred_element_type=jnp.float32)
            b = jnp.dot(x, wub[s, :, cols], preferred_element_type=jnp.float32)
            h = jax.nn.silu(a) * b
            for i, block in enumerate(blocks):
                live = row < fill[e, dev(*block)]
                hid[i * cap:(i + 1) * cap, cols] = jnp.where(live, h[i * cap:(i + 1) * cap], 0.0).astype(jnp.bfloat16)

    def leaf_copy(i, e, c):
        a, rel = BLOCKS_L[i]
        return remote(lsend.at[i, e, c], leaf.at[i % 2, c, rows_of(rel, e)], lsend_sem,
                      leaf_sem.at[i % 2, c], dev(1 if a > 0 else -1, rel))

    def sibling_copy(cls, e):
        return remote(ysend.at[cls, e], ybuf.at[cls, :, rows_of(1, e)], ysend_sem, ybuf_sem.at[cls], dev(0, 1))

    def down_phase(e, blocks, wait, after=None):
        s = lax.rem(e, 2)
        leaves = blocks is BLOCKS_L

        for n in range(chunks):
            if wait:
                d_copy(e, n).wait()
            if after is not None and n == 0:
                after()
            y = jnp.dot(hid[...], wdb[s, :, columns(n)], preferred_element_type=jnp.float32).astype(jnp.bfloat16)
            for i, (a, rel) in enumerate(blocks):
                block = y[i * cap:(i + 1) * cap]
                if leaves:
                    lsend[i, e, n] = block
                elif rel == 0:
                    ybuf[CLASS[a], n, rows_of(0, e)] = block
                else:
                    ysend[CLASS[a], e, n] = block
            if leaves:
                for i in range(len(blocks)):
                    leaf_copy(i, e, n).start()
        if not leaves:
            for a, rel in blocks:
                if rel == 1:
                    sibling_copy(CLASS[a], e).start()

    meta_to = [(-3, 0), (2, 1), (-2, 2), (1, 3), (-1, 4)]

    def meta_copy(a, cls):
        return remote(meta.at[rows_meta(CLASS[0])], meta.at[rows_meta(cls)], msend_sem, meta_sem.at[0], dev(a, 0))

    def load_next(e):
        start_x(0, e)
        start_gu(e)
        start_d(e)
        start_x(1, e)

    def rest_unit(e):
        wait_x(1, e)
        up_phase(xa.at[1, e], e, BLOCKS_R, False)
        down_phase(e, BLOCKS_R, False)

    def early_unit(e, carry):
        def following():
            @pl.when(e + 1 < experts)
            def _():
                load_next(e + 1)

        wait_x(0, e)
        up_phase(xa.at[0, e], e, BLOCKS_L, True)
        down_phase(e, BLOCKS_L, True, following)
        rest_unit(e)
        return carry

    wait_x(0, 0)
    up_phase(xa.at[0, 0], 0, BLOCKS_L, True, lambda: start_d(0))
    pl.semaphore_wait(barrier, len(partners))
    for a, cls in meta_to:
        meta_copy(a, cls).start()
    start_x(1, 0)
    down_phase(0, BLOCKS_L, True, lambda: load_next(1))
    rest_unit(0)
    lax.fori_loop(1, 2, early_unit, 0)

    arrived(meta.at[pl.ds(0, 2 * top_k * len(meta_to))], meta_sem.at[0])
    scr[...] = meta[...].T
    col = lax.broadcasted_iota(jnp.int32, (tokens, 2 * per_core), 1)
    order = lax.rem(col + k * per_core, 2 * per_core)

    def select(where, cls, a_chip):
        chip = lax.rem(z + a_chip * sigma + zn, zn)
        want = (order + chip * (2 * per_core)).astype(jnp.float32)
        weight = jnp.zeros((tokens, 2 * per_core), jnp.float32)
        for j in range(top_k):
            c = 2 * top_k * cls + j
            weight = jnp.where(scr[:, c:c + 1] == want, scr[:, c + top_k:c + top_k + 1], weight)
        for i in range(3):
            piece = weight.astype(jnp.bfloat16)
            sel[where, i * tokens:(i + 1) * tokens] = piece
            weight = weight - piece.astype(jnp.float32)

    for cls in (0, 1):
        select(cls, cls, 0)
        select(6 + cls, cls, -1 if cls == 0 else 1)

    lax.fori_loop(2, experts, early_unit, 0)
    for e in range(experts):
        start_x(2, e)


    def weigh(where, rows_ref):
        p = jnp.dot(sel[where], rows_ref[...], preferred_element_type=jnp.float32)
        return p[0:tokens] + p[tokens:2 * tokens] + p[2 * tokens:3 * tokens]

    def part_copy(src, to, c, a):
        return remote(src, part.at[to, c], head_sem if to < 2 else psend_sem, part_sem.at[to, c], dev(a, 0))

    def wait_part(to, c):
        arrived(part.at[to, c], part_sem.at[to, c])

    def wait_sibling(cls):
        arrived(ybuf.at[cls, :, pl.ds(per_core, per_core)], ybuf_sem.at[cls])


    for cls in (0, 1):
        wait_sibling(cls)

    def second(c, carry):
        for i in range(2):
            mine = weigh(i, ybuf.at[i, c])
            arrived(leaf.at[i, c], leaf_sem.at[i, c])
            head[i, c] = mine + weigh(6 + i, leaf.at[i, c])
            part_copy(head.at[i, c], i, c, 1 if i == 0 else -1).start()
        return carry

    lax.fori_loop(0, chunks, second, 0)

    def later_unit(p, half):
        def body(q, carry):
            e = q + 2 * ((p + half + 1) % 2)
            up_phase(xb.at[p, e], e, BLOCKS_B[p], half == 1)
            if half == 0:
                start_gu(lax.rem(e + 2, experts))
            down_phase(e, BLOCKS_B[p], half == 1)
            if half == 0:
                start_d(lax.rem(e + 2, experts))
            return carry
        return body

    def later_pass(p):
        arrived(xb.at[p], x_sem.at[2 + p, 0])
        for half in range(2):
            lax.fori_loop(0, 2, later_unit(p, half), 0)

    for cls in range(2, 6):
        select(cls, cls, 0)
    for e in range(experts):
        start_x(3, e)
    later_pass(0)
    wait_sibling(2)
    wait_sibling(3)

    def third(c, carry):
        for i in range(2):
            mine = weigh(2 + i, ybuf.at[2 + i, c])
            way = 1 if i == 0 else -1
            wait_part(i, c)
            part[i, c] = part[i, c] + mine
            part_copy(part.at[i, c], 2 + i, c, way).start()
        return carry

    lax.fori_loop(0, chunks, third, 0)

    later_pass(1)
    wait_sibling(4)
    wait_sibling(5)

    def fourth(c, carry):
        mine = weigh(4, ybuf.at[4, c])
        wait_part(2, c)
        part[2, c] = part[2, c] + mine
        part_copy(part.at[2, c], 4, c, 1).start()
        return carry

    lax.fori_loop(0, chunks, fourth, 0)

    def out_copy(c):
        return pltpu.make_async_copy(outv.at[c], out.at[:, columns(c)], out_sem.at[0])

    def last(c, carry):
        mine = weigh(5, ybuf.at[5, c])
        wait_part(3, c)
        mine = mine + part[3, c]
        wait_part(4, c)
        outv[c] = (mine + part[4, c]).astype(out.dtype)
        out_copy(c).start()
        return carry

    lax.fori_loop(0, chunks, last, 0)

    arrived(outv, out_sem.at[0])
    arrived(meta.at[pl.ds(0, 2 * top_k * len(meta_to))], msend_sem)
    arrived(lsend, lsend_sem)
    arrived(ysend, ysend_sem)
    arrived(head, head_sem)
    arrived(part.at[pl.ds(0, 3)], psend_sem)


def solution(mesh):
    zn = mesh.shape["ep"] // 2

    def local_step(dispatched, w_gate, w_up, w_down, fill_count, slot_index, expert_id, gate_weight):
        sources, experts, cap, dim = dispatched.shape
        ffn = w_gate.shape[2]
        tokens = slot_index.shape[0]
        bf16, f32 = jnp.bfloat16, jnp.float32
        width = TILE
        chunks = dim // width
        blocks = len(BLOCKS_L)
        rows = blocks * cap
        any_spec = pl.BlockSpec(memory_space=pl.ANY)
        dma = pltpu.SemaphoreType.DMA
        return pl.pallas_call(
            functools.partial(kernel, zn),
            out_shape=jax.ShapeDtypeStruct((tokens, dim), bf16),
            in_specs=[any_spec] * 8,
            out_specs=any_spec,
            scratch_shapes=[
                pltpu.VMEM((2, experts, rows, dim), bf16),
                pltpu.VMEM((2, experts, rows, dim), bf16),
                pltpu.VMEM((2, dim, ffn), bf16),
                pltpu.VMEM((2, dim, ffn), bf16),
                pltpu.VMEM((2, ffn, dim), bf16),
                pltpu.VMEM((rows, ffn), bf16),
                pltpu.VMEM((blocks, experts, chunks, cap, width), bf16),
                pltpu.VMEM((2, chunks, 2 * experts * cap, width), bf16),
                pltpu.VMEM((6, experts, chunks, cap, width), bf16),
                pltpu.VMEM((6, chunks, 2 * experts * cap, width), bf16),
                pltpu.VMEM((2, chunks, tokens, width), f32),
                pltpu.VMEM((5, chunks, tokens, width), f32),
                pltpu.VMEM((128, tokens), f32),
                pltpu.VMEM((128, 128), f32),
                pltpu.VMEM((8, 3 * tokens, 2 * experts * cap), bf16),
                pltpu.VMEM((chunks, tokens, width), bf16),
                pltpu.SMEM((experts, sources), jnp.int32),
                pltpu.VMEM(slot_index.shape[::-1], jnp.int32),
                pltpu.VMEM(expert_id.shape[::-1], jnp.int32),
                pltpu.VMEM(gate_weight.shape[::-1], f32),
                dma((4, experts)),
                dma((2, 2, ffn // UP_TILE)),
                dma((2, chunks)),
                dma((4,)),
                dma((2, chunks)),
                dma((6,)),
                dma((5, chunks)),
                dma((1,)),
                dma((5,)),
                dma((1,)),
            ],
            compiler_params=pltpu.CompilerParams(
                collective_id=0, has_side_effects=True, vmem_limit_bytes=67043328),
        )(dispatched, w_gate, w_up, w_down, fill_count.T, slot_index.T, expert_id.T, gate_weight.T)

    token_spec = P(("dp", "ep"))
    in_specs = (P("dp", "ep"), P("ep"), P("ep"), P("ep"), P("dp", "ep"), token_spec, token_spec, token_spec)
    return jax.shard_map(local_step, mesh=mesh, in_specs=in_specs, out_specs=token_spec, check_vma=False)
```
